16 devices in a mesh: dp: 2 (over y, z), tp: 8 (over x, core).
Axes of the slice: x: 4, y: 2, z: 1, core: 2. Of those that a mesh axis runs over, the one named last changes fastest.
The devices are a block of a 4x4x8 slice.
Arguments:
- x: bfloat16 [8192, 2048], P(('dp', 'tp')), parts along dimension 0
- gain_a: bfloat16 [2048], replicated
- wq: bfloat16 [2048, 2048], P(None, 'tp')
- wk: bfloat16 [2048, 2048], P(None, 'tp')
- wv: bfloat16 [2048, 2048], P(None, 'tp')
- wo: bfloat16 [2048, 2048], P('tp')
- gain_m: bfloat16 [2048], replicated
- w_gate: bfloat16 [2048, 8192], P(None, 'tp')
- w_up: bfloat16 [2048, 8192], P(None, 'tp')
- w_down: bfloat16 [8192, 2048], P('tp')
Outputs:
- output: bfloat16 [8192, 2048], P(('dp', 'tp')), parts along dimension 0
There are 2 independent parts. The reference program is written for one: setup_inputs(seed, part) draws one part's arguments, and reference() takes and returns one part's arrays. A program takes and returns all parts, laid end to end along the dimension named above; an argument that names none is the same for every part.
All inputs are finite; a program needn't handle non-finite values.
Results may differ from the reference program's by a relative error of at most 0.017.
Values are sent between devices in bfloat16 or wider.
A program may use at most 768 MiB of HBM per device.

```python
import jax
import jax.numpy as jnp
from jax import lax

ROWS = 4096
D = 2048
HEADS = 16
KV_HEADS = 16
HEAD = 128
FF = 8192
THETA = 10000


def setup_inputs(seed: int = 0, part: int = 0) -> dict:
    kx, kn, kq, kk, kv, ko, km, kg, ku, kd = jax.random.split(jax.random.key(seed), 10)

    def weights(key, rows, columns):
        return jax.random.normal(key, (rows, columns), jnp.float32) * rows**-0.5

    drawn = {
        "x": jax.random.normal(jax.random.fold_in(kx, part), (ROWS, D), jnp.float32),
        "gain_a": 1 + 0.1 * jax.random.normal(kn, (D,), jnp.float32),
        "wq": 2 * weights(kq, D, HEADS * HEAD),
        "wk": 2 * weights(kk, D, KV_HEADS * HEAD),
        "wv": 4 * weights(kv, D, KV_HEADS * HEAD),
        "wo": weights(ko, HEADS * HEAD, D),
        "gain_m": 1 + 0.1 * jax.random.normal(km, (D,), jnp.float32),
        "w_gate": weights(kg, D, FF),
        "w_up": weights(ku, D, FF),
        "w_down": 2 * weights(kd, FF, D),
    }
    return {k: v.astype(jnp.bfloat16) for k, v in drawn.items()}


def normed(x, gain):
    wide = x.astype(jnp.float32)
    scale = lax.rsqrt(jnp.mean(wide * wide, -1, keepdims=True) + 1e-6)
    return (wide * scale * gain.astype(jnp.float32)).astype(jnp.bfloat16)


def turned(t, place, theta):
    half = t.shape[-1] // 2
    angle = place.astype(jnp.float32)[:, None] * theta ** (-jnp.arange(half, dtype=jnp.float32) / half)
    cos, sin = jnp.cos(angle)[:, None], jnp.sin(angle)[:, None]
    a, b = t[..., :half].astype(jnp.float32), t[..., half:].astype(jnp.float32)
    return jnp.concatenate([a * cos - b * sin, b * cos + a * sin], -1).astype(jnp.bfloat16)


def matmul(a, w):
    return jnp.dot(a, w, preferred_element_type=jnp.float32).astype(jnp.bfloat16)


def einsum(form, a, b):
    return jnp.einsum(form, a.astype(jnp.float32), b.astype(jnp.float32))


def attention(q, k, v):
    scores = einsum("tgsd,ugd->gstu", q, k) * q.shape[-1] ** -0.5
    token = jnp.arange(q.shape[0])
    scores = jnp.where(token[:, None] >= token, scores, -jnp.inf)
    weights = jax.nn.softmax(scores, -1).astype(jnp.bfloat16)
    return einsum("gstu,ugd->tgsd", weights, v).astype(jnp.bfloat16)


def reference(x, gain_a, wq, wk, wv, wo, gain_m, w_gate, w_up, w_down):
    a, place = normed(x, gain_a), jnp.arange(ROWS)
    q = turned(matmul(a, wq).reshape(ROWS, HEADS, HEAD), place, THETA).reshape(ROWS, KV_HEADS, -1, HEAD)
    k = turned(matmul(a, wk).reshape(ROWS, KV_HEADS, HEAD), place, THETA)
    v = matmul(a, wv).reshape(ROWS, KV_HEADS, HEAD)
    seen = attention(q, k, v).reshape(ROWS, HEADS * HEAD)
    h = (x.astype(jnp.float32) + jnp.dot(seen, wo, preferred_element_type=jnp.float32)).astype(jnp.bfloat16)
    b = normed(h, gain_m)
    gate = jnp.dot(b, w_gate, preferred_element_type=jnp.float32)
    up = jnp.dot(b, w_up, preferred_element_type=jnp.float32)
    hidden = (jax.nn.silu(gate) * up).astype(jnp.bfloat16)
    return (h.astype(jnp.float32) + jnp.dot(hidden, w_down, preferred_element_type=jnp.float32)).astype(jnp.bfloat16)
```

```python
import functools

import jax
import jax.numpy as jnp
import numpy as np
from jax import lax
from jax.experimental import pallas as pl
from jax.experimental.pallas import tpu as pltpu
from jax.sharding import PartitionSpec as P

MESH = pl.DeviceIdType.MESH
HEAD = 128
THETA = 10000
NEG = -1e30
HIDDEN = 2 * NEG
LOG2E = 1.4426950408889634
CHUNKS = 4
LIMIT = 67_000_000


def normed(x, gain):
    wide = x.astype(jnp.float32)
    scale = lax.rsqrt(jnp.mean(wide * wide, -1, keepdims=True) + 1e-6)
    return (wide * scale * gain.astype(jnp.float32)).astype(jnp.bfloat16)


def dot(a, b, ca=1, cb=0):
    return lax.dot_general(a, b, (((ca,), (cb,)), ((), ())), preferred_element_type=jnp.float32)


def sending(src, dst, send_sem, recv_sem, device):
    return pltpu.make_async_remote_copy(
        src_ref=src, dst_ref=dst, send_sem=send_sem, recv_sem=recv_sem, device_id={"tp": device}, device_id_type=MESH
    )


def landed(dst, sem):
    pltpu.make_async_copy(dst, dst, sem).wait()


class Place:
    def __init__(self, n):
        self.n = n
        self.me = lax.axis_index("tp")
        self.core = lax.rem(self.me, 2)
        self.chip = lax.div(self.me, 2)
        self.sib = self.me + 1 - 2 * self.core
        self.right, self.left, self.far = (lax.rem(self.me + 2 * k, n) for k in (1, n // 2 - 1, 2))

    def at(self, off, other=0):
        return lax.rem(self.chip + off, self.n // 2) * 2 + lax.rem(self.core + other, 2)


def greet(devices):
    barrier = pltpu.get_barrier_semaphore()
    for d in devices:
        pl.semaphore_signal(barrier, inc=1, device_id={"tp": d}, device_id_type=MESH)
    pl.semaphore_wait(barrier, len(devices))


class Gather:
    def __init__(self, at, slots, recv, to_right, to_left, to_sib):
        self.at, self.slots, self.recv, self.to_right, self.to_left, self.to_sib = at, slots, recv, to_right, to_left, to_sib
        self.rows = slots.shape[1] // CHUNKS

    def piece(self, block, c):
        return self.slots.at[block, pl.ds(c * self.rows, self.rows), :]

    def send(self, block, c, sem, device):
        sending(self.piece(block, c), self.piece(block, c), sem, self.recv.at[block, c], device).start()

    def wait(self, block, c):
        landed(self.piece(block, c), self.recv.at[block, c])

    def start(self, x_ref, gain_ref):
        at, me = self.at, self.at.me

        def norm(c):
            here = pl.ds(c * self.rows, self.rows)
            self.slots[me, here, :] = normed(x_ref[here, :], gain_ref[...])

        right = lambda c: self.send(me, c, self.to_right.at[c], at.right)
        left = lambda c: self.send(me, c, self.to_left.at[c], at.left)
        sib = lambda c: self.send(me, c, self.to_sib.at[c], at.sib)
        norm(0)
        norm(2)
        right(0), sib(0)
        norm(1)
        left(2), sib(2)
        norm(3)
        right(1), sib(1)
        left(3), sib(3)
        right(2), left(0), right(3), left(1)

    def step(self, s):
        at = self.at
        if s < 4:
            a, b, i, j = at.left, at.right, s, (s + 2) % 4
            ka, kb = 1, 2
        else:
            a, b, i, j = at.far, at.far, s - 4, s - 2
            ka, kb = 3, 3
        self.wait(a, i)
        if s < 2:
            self.send(a, i, self.to_right.at[CHUNKS + s], at.right)
        self.send(a, i, self.to_sib.at[CHUNKS * ka + i], at.sib)
        self.wait(b, j)
        if s < 2:
            self.send(b, j, self.to_left.at[CHUNKS + s], at.left)
        self.send(b, j, self.to_sib.at[CHUNKS * kb + j], at.sib)
        return i, j

    def left_own(self):
        for c in range(CHUNKS):
            for sems in (self.to_right, self.to_left, self.to_sib):
                landed(self.piece(self.at.me, c), sems.at[c])

    def left_rest(self):
        for c in range(2):
            for sems in (self.to_right, self.to_left):
                landed(self.piece(self.at.me, c), sems.at[CHUNKS + c])
        for c in range(CHUNKS, 4 * CHUNKS):
            landed(self.piece(self.at.me, 0), self.to_sib.at[c])


GATHER_SEMS = [
    pltpu.SemaphoreType.DMA((8, CHUNKS)),
    pltpu.SemaphoreType.DMA((CHUNKS + 2,)),
    pltpu.SemaphoreType.DMA((CHUNKS + 2,)),
    pltpu.SemaphoreType.DMA((4 * CHUNKS,)),
]


def attention_half(n, x_ref, gain_ref, wq_hbm, wk_hbm, wv_hbm, wo_hbm, row_ref, block_ref, h_ref,
                   slots, wq_s, wk_s, wv_s, wo_s, q_s, k_s, v_s, top_s, mix_s, seen_s, got_s,
                   recv, to_right, to_left, to_sib, wo_recv, wo_right, wo_left, wo_sib, all_send, all_recv, local):
    at = Place(n)
    me = at.me
    rows = x_ref.shape[0]
    loads = [pltpu.make_async_copy(a, b, local.at[i]) for i, (a, b) in
             enumerate(((wq_hbm, wq_s), (wk_hbm, wk_s), (wv_hbm, wv_s), (wo_hbm, wo_s.at[me])))]
    for load in loads:
        load.start()
    greet([lax.rem(me + k, n) for k in range(1, n)])
    g = Gather(at, slots, recv, to_right, to_left, to_sib)
    g.start(x_ref, gain_ref)
    for h in range(2):
        v_s[h, HEAD:, :] = jnp.ones((8, v_s.shape[2]), jnp.bfloat16)
    for load in loads[:3]:
        load.wait()
    size = g.rows
    sign = jnp.where(lax.broadcasted_iota(jnp.int32, (1, HEAD), 1) < HEAD // 2, -1.0, 1.0)

    def project(b, c):
        here = pl.ds(pl.multiple_of(c * size, size), size)
        there = pl.ds(pl.multiple_of(b * rows + c * size, size), size)
        a = slots[b, here, :]
        cr, sr = row_ref[0, here, :], row_ref[1, here, :]
        cb, sb = block_ref[0, pl.ds(b, 1), :], block_ref[1, pl.ds(b, 1), :]
        cos, sin = cr * cb - sr * sb, (sr * cb + cr * sb) * sign
        for w, out in ((wq_s, q_s), (wk_s, k_s)):
            t = dot(a, w[...]).astype(jnp.bfloat16).astype(jnp.float32)
            for h in range(2):
                one = t[:, h * HEAD : (h + 1) * HEAD]
                turned = one * cos + pltpu.roll(one, HEAD // 2, 1) * sin
                out[h, there, :] = turned.astype(jnp.bfloat16)
        t = dot(a, wv_s[...])
        for h in range(2):
            v_s[h, :HEAD, there] = t[:, h * HEAD : (h + 1) * HEAD].T.astype(jnp.bfloat16)

    for c in range(CHUNKS):
        g.wait(at.sib, c)
    lax.fori_loop(0, 2 * CHUNKS, lambda i, _: project(at.at(0, lax.div(i, CHUNKS)), lax.rem(i, CHUNKS)), None)
    loads[3].wait()

    def wo_piece(b, c):
        return wo_s.at[b, pl.ds(c * HEAD, HEAD), :]

    def wo_send(b, c, sem, device):
        sending(wo_piece(b, c), wo_piece(b, c), sem, wo_recv.at[b, c], device).start()

    def wo_wait(b, c):
        landed(wo_piece(b, c), wo_recv.at[b, c])

    for s in range(6):
        i, j = g.step(s)
        if s == 4:
            wo_send(me, 0, wo_right.at[0], at.right)
            wo_send(me, 1, wo_left.at[1], at.left)
            wo_send(me, 1, wo_right.at[1], at.right)
            wo_send(me, 0, wo_left.at[0], at.left)
            for c in range(2):
                wo_send(me, c, wo_sib.at[c], at.sib)
        off = (lambda k: n // 2 - 1 + 2 * k) if s < 4 else (lambda k: 2)
        g.wait(at.at(off(0), 1), i)
        g.wait(at.at(off(1), 1), j)
        lax.fori_loop(0, 4, lambda k, _: project(at.at(off(lax.rem(k, 2)), lax.div(k, 2)), i + lax.rem(k, 2) * (j - i)), None)

    e = HEAD**-0.5 * LOG2E

    def attend(key, b, strips, masked):
        here = pl.ds(pl.multiple_of(key * rows, rows), rows)
        pieces = [(h, i) for i in strips for h in range(2)]
        scores = [dot(k_s[h, here, :], q_s[h, pl.ds(pl.multiple_of((b + i) * rows, rows), rows), :], 1, 1) for h, i in pieces]
        weights, keeps = [], []
        for (h, i), s in zip(pieces, scores):
            if i in masked:
                ok = lax.broadcasted_iota(jnp.int32, s.shape, 1) >= lax.broadcasted_iota(jnp.int32, s.shape, 0)
                s = jnp.where(ok, s, HIDDEN)
            r = 2 * i + h
            old = top_s[r : r + 1, :]
            top = jnp.maximum(old, s.max(axis=0, keepdims=True))
            top_s[r : r + 1, :] = top
            weights.append(jnp.exp2((s - top) * e).astype(jnp.bfloat16))
            keeps.append(jnp.exp2((old - top) * e))
        for (h, i), p, keep in zip(pieces, weights, keeps):
            r = 2 * i + h
            mix_s[r] = mix_s[r] * keep + dot(v_s[h, :, here], p)

    def share(d):
        sending(seen_s.at[d], got_s.at[me], all_send.at[d], all_recv.at[me], d).start()

    def turn(t, _):
        b = lax.rem(at.chip + t + 1, n // 2) * 2
        top_s[...] = jnp.full(top_s.shape, NEG, jnp.float32)
        mix_s[...] = jnp.zeros(mix_s.shape, jnp.float32)
        lax.fori_loop(0, b, lambda key, _: attend(key, b, (0, 1), ()), None)
        attend(b, b, (0, 1), (0,))
        attend(b + 1, b, (1,), (1,))
        for i in range(2):
            for h in range(2):
                m = mix_s[2 * i + h]
                o = m[:HEAD] * (1 / m[HEAD : HEAD + 1])
                seen_s[b + i, :, h * HEAD : (h + 1) * HEAD] = o.T.astype(jnp.bfloat16)

        @pl.when(t == 0)
        def _():
            wo_wait(at.left, 0)
            wo_send(at.left, 0, wo_right.at[2], at.right)
            wo_send(at.left, 0, wo_sib.at[2], at.sib)
            wo_wait(at.right, 1)
            wo_send(at.right, 1, wo_left.at[2], at.left)
            wo_send(at.right, 1, wo_sib.at[5], at.sib)

        @pl.when(t == 1)
        def _():
            wo_wait(at.left, 1)
            wo_send(at.left, 1, wo_sib.at[3], at.sib)
            wo_wait(at.right, 0)
            wo_send(at.right, 0, wo_sib.at[4], at.sib)

        @pl.when(t < n // 2 - 1)
        def _():
            share(b)
            share(b + 1)

    lax.fori_loop(0, n // 2, turn, None)
    share(at.sib)
    for c in range(2):
        wo_wait(at.far, c)
        wo_send(at.far, c, wo_sib.at[6 + c], at.sib)
    got_s[me] = seen_s[me]
    for off in range(n // 2):
        for c in range(2):
            wo_wait(at.at(off, 1), c)
    for k in range(1, n):
        b = lax.rem(me + k, n)
        landed(got_s.at[b], all_recv.at[b])
    wide = 512

    def out(t, _):
        here = pl.ds(pl.multiple_of(t * wide, wide), wide)
        total = dot(got_s[0], wo_s[0, :, here])
        for b in range(1, n):
            total += dot(got_s[b], wo_s[b, :, here])
        h_ref[:, here] = (x_ref[:, here].astype(jnp.float32) + total).astype(jnp.bfloat16)

    lax.fori_loop(0, h_ref.shape[1] // wide, out, None)
    g.left_own()
    g.left_rest()
    for c in range(3):
        landed(wo_piece(me, 0), wo_right.at[c])
        landed(wo_piece(me, 0), wo_left.at[c])
    for c in range(8):
        landed(wo_piece(me, 0), wo_sib.at[c])
    for k in range(1, n):
        d = lax.rem(me + k, n)
        landed(seen_s.at[d], all_send.at[d])


def mlp_half(n, h_ref, gain_ref, wg_hbm, wu_hbm, wd_hbm, y_ref,
             slots, wg_s, wu_s, wd_s, hid_s, term_s, run_s, from_s,
             recv, to_right, to_left, to_sib, term_send, term_recv, ring_send, ring_recv, local):
    at = Place(n)
    me = at.me
    rows, d = h_ref.shape
    half, wide = rows // 2, d // 2
    loads = [pltpu.make_async_copy(a, b, local.at[i]) for i, (a, b) in enumerate(((wg_hbm, wg_s), (wu_hbm, wu_s), (wd_hbm, wd_s)))]
    for load in loads:
        load.start()
    greet([at.sib, at.right, at.left])
    g = Gather(at, slots, recv, to_right, to_left, to_sib)
    g.start(h_ref, gain_ref)
    loads[0].wait()
    loads[1].wait()
    cut = 256
    cuts = hid_s.shape[2] // cut

    def hidden(b, part, t):
        here = pl.ds(pl.multiple_of(part * half, half), half)
        cols = pl.ds(pl.multiple_of(t * cut, cut), cut)
        a = slots[b, here, :]
        gate, up = dot(a, wg_s[:, cols]), dot(a, wu_s[:, cols])
        hid_s[b, here, cols] = (jax.nn.silu(gate) * up).astype(jnp.bfloat16)

    def four(off, part):
        def one(i, _):
            k, t = lax.div(i, cuts), lax.rem(i, cuts)
            side = lax.rem(k, 2)
            hidden(at.at(off(side), lax.div(k, 2)), part(side), t)
        lax.fori_loop(0, 4 * cuts, one, None)

    for c in range(CHUNKS):
        g.wait(at.sib, c)
    four(lambda side: 0, lambda side: side)

    def piece(ref, index, part, c):
        return ref.at[(*index, pl.ds(pl.multiple_of(part * half, half), half), pl.ds(pl.multiple_of(c * wide, wide), wide))]

    def term(b, part, c):
        rows_ = pl.ds(pl.multiple_of(part * half, half), half)
        return dot(hid_s[b, rows_, :], wd_s[:, pl.ds(pl.multiple_of(c * wide, wide), wide)])

    def chips_term(k, off, part, i, c):
        other = at.at(off, 1)
        source = piece(slots, (other,), part, c)
        source[...] = term(other, part, c).astype(jnp.bfloat16)
        mine = term(at.at(off), part, c)
        target = piece(term_s, (k, i), 0, c)
        sending(source, target, term_send.at[k, i, c], term_recv.at[k, i, c], at.sib).start()
        landed(target, term_recv.at[k, i, c])
        return mine + target[...].astype(jnp.float32)

    def group(k, off, part, stage, extra=False):
        def ring(index):
            c, i = lax.div(index, 2), lax.rem(index, 2)
            source = piece(slots, (stage(i),), part(i), c)
            target = piece(run_s, (i,), 0, c) if k == 1 else piece(from_s, (i,), part(i), c)
            return sending(source, target, ring_send.at[k, i, c], ring_recv.at[k, i, c], lax.rem(me + 2 + (n - 4) * i, n))

        def one(index, _):
            c, i = lax.div(index, 2), lax.rem(index, 2)
            total = chips_term(k, off(i), part(i), i, c)
            if extra:
                came = piece(run_s, (i,), 0, c)
                landed(came, ring_recv.at[1, i, c])
                total += came[...].astype(jnp.float32)
            piece(slots, (stage(i),), part(i), c)[...] = total.astype(jnp.bfloat16)
            ring(index).start()

        lax.fori_loop(0, 4, one, None)

    near = lambda side: n // 2 - 1 + 2 * side
    turned = lambda i: 1 + (n // 2 - 2) * i
    for s in range(6):
        i, j = g.step(s)
        off = near if s < 4 else (lambda side: 2)
        if s % 2:
            for c in (i - 1, i):
                g.wait(at.at(off(0), 1), c)
            for c in (j - 1, j):
                g.wait(at.at(off(1), 1), c)
            first, last = i // 2, j // 2
            four(off, lambda side: first + side * (last - first))
        if s == 3:
            loads[2].wait()
            g.left_own()
            group(0, turned, lambda i: 1 - i, lambda i: me)
    g.left_rest()
    group(1, lambda i: 2, lambda i: i, lambda i: at.far)
    group(2, turned, lambda i: i, lambda i: at.at(turned(i)), extra=True)

    def last(index, _):
        c, i = lax.div(index, 2), lax.rem(index, 2)
        total = chips_term(3, 0, i, i, c)
        for side in range(2):
            came = piece(from_s, (side,), i, c)
            kind = 2 * (1 - i) if side == 0 else 2 * i
            landed(came, ring_recv.at[kind, side, c])
            total += came[...].astype(jnp.float32)
        here = piece(h_ref, (), i, c)
        piece(y_ref, (), i, c)[...] = (here[...].astype(jnp.float32) + total).astype(jnp.bfloat16)

    lax.fori_loop(0, 4, last, None)
    sample = piece(slots, (me,), 0, 0)
    for i in range(2):
        for c in range(2):
            for k in range(4):
                landed(sample, term_send.at[k, i, c])
            for k in range(3):
                landed(sample, ring_send.at[k, i, c])


def tables(rows, n):
    freq = float(THETA) ** (-np.arange(HEAD // 2) / (HEAD // 2))

    def both(place):
        angle = np.tile(place[:, None] * freq, (1, 2))
        return jnp.asarray(np.stack([np.cos(angle), np.sin(angle)]).astype(np.float32))

    return both(np.arange(rows)), both(np.arange(n) * rows)


def solution(mesh):
    n = mesh.shape["tp"]
    vmem, hbm = pl.BlockSpec(memory_space=pltpu.VMEM), pl.BlockSpec(memory_space=pl.ANY)
    dma = pltpu.SemaphoreType.DMA
    bf16 = jnp.bfloat16

    def step(x, gain_a, wq, wk, wv, wo, gain_m, w_gate, w_up, w_down):
        rows, d = x.shape
        width, units = wq.shape[1], w_gate.shape[1]
        row_table, block_table = tables(rows, n)
        h = pl.pallas_call(
            functools.partial(attention_half, n),
            name="attention_half",
            out_shape=jax.ShapeDtypeStruct((rows, d), bf16),
            in_specs=[vmem, vmem, hbm, hbm, hbm, hbm, vmem, vmem],
            out_specs=vmem,
            scratch_shapes=[
                pltpu.VMEM((n, rows, d), bf16),
                pltpu.VMEM((d, width), bf16),
                pltpu.VMEM((d, width), bf16),
                pltpu.VMEM((d, width), bf16),
                pltpu.VMEM((n, width, d), bf16),
                pltpu.VMEM((2, n * rows, HEAD), bf16),
                pltpu.VMEM((2, n * rows, HEAD), bf16),
                pltpu.VMEM((2, HEAD + 8, n * rows), bf16),
                pltpu.VMEM((4, rows), jnp.float32),
                pltpu.VMEM((4, HEAD + 8, rows), jnp.float32),
                pltpu.VMEM((n, rows, width), bf16),
                pltpu.VMEM((n, rows, width), bf16),
                *GATHER_SEMS,
                dma((n, 2)), dma((3,)), dma((3,)), dma((8,)), dma((n,)), dma((n,)), dma((4,)),
            ],
            compiler_params=pltpu.CompilerParams(collective_id=0, has_side_effects=True, vmem_limit_bytes=LIMIT),
        )(x, gain_a[None], wq, wk, wv, wo, row_table, block_table)
        return pl.pallas_call(
            functools.partial(mlp_half, n),
            name="mlp_half",
            out_shape=jax.ShapeDtypeStruct((rows, d), bf16),
            in_specs=[vmem, vmem, hbm, hbm, hbm],
            out_specs=vmem,
            scratch_shapes=[
                pltpu.VMEM((n, rows, d), bf16),
                pltpu.VMEM((d, units), bf16),
                pltpu.VMEM((d, units), bf16),
                pltpu.VMEM((units, d), bf16),
                pltpu.VMEM((n, rows, units), bf16),
                pltpu.VMEM((4, 2, rows // 2, d), bf16),
                pltpu.VMEM((2, rows // 2, d), bf16),
                pltpu.VMEM((2, rows, d), bf16),
                *GATHER_SEMS,
                dma((4, 2, 2)), dma((4, 2, 2)), dma((3, 2, 2)), dma((3, 2, 2)), dma((3,)),
            ],
            compiler_params=pltpu.CompilerParams(collective_id=1, has_side_effects=True, vmem_limit_bytes=LIMIT),
        )(h, gain_m[None], w_gate, w_up, w_down)

    tokens, columns, rows_of = P(("dp", "tp"), None), P(None, "tp"), P("tp", None)
    return jax.shard_map(
        step,
        mesh=mesh,
        in_specs=(tokens, P(None), columns, columns, columns, rows_of, P(None), columns, columns, rows_of),
        out_specs=tokens,
        check_vma=False,
    )
```

```python
import functools

import jax
import jax.numpy as jnp
import numpy as np
from jax import lax
from jax.experimental import pallas as pl
from jax.experimental.pallas import tpu as pltpu
from jax.sharding import PartitionSpec as P

MESH = pl.DeviceIdType.MESH
HEAD = 128
THETA = 10000
NEG = -1e30
HIDDEN = 2 * NEG
LOG2E = 1.4426950408889634
CHUNKS = 4
LIMIT = 67_000_000


def normed(x, gain):
    wide = x.astype(jnp.float32)
    scale = lax.rsqrt(jnp.mean(wide * wide, -1, keepdims=True) + 1e-6)
    return (wide * scale * gain.astype(jnp.float32)).astype(jnp.bfloat16)


def dot(a, b, ca=1, cb=0):
    return lax.dot_general(a, b, (((ca,), (cb,)), ((), ())), preferred_element_type=jnp.float32)


def sending(src, dst, send_sem, recv_sem, device):
    return pltpu.make_async_remote_copy(
        src_ref=src, dst_ref=dst, send_sem=send_sem, recv_sem=recv_sem, device_id={"tp": device}, device_id_type=MESH
    )


def landed(dst, sem):
    pltpu.make_async_copy(dst, dst, sem).wait()


class Place:
    def __init__(self, n):
        self.n = n
        self.me = lax.axis_index("tp")
        self.core = lax.rem(self.me, 2)
        self.chip = lax.div(self.me, 2)
        self.sib = self.me + 1 - 2 * self.core
        self.right, self.left, self.far = (lax.rem(self.me + 2 * k, n) for k in (1, n // 2 - 1, 2))

    def at(self, off, other=0):
        return lax.rem(self.chip + off, self.n // 2) * 2 + lax.rem(self.core + other, 2)


class Gather:
    def __init__(self, at, slots, recv, to_right, to_left, to_sib):
        self.at, self.slots, self.recv, self.to_right, self.to_left, self.to_sib = at, slots, recv, to_right, to_left, to_sib
        self.rows = slots.shape[1] // CHUNKS

    def piece(self, block, c):
        return self.slots.at[block, pl.ds(c * self.rows, self.rows), :]

    def send(self, block, c, sem, device):
        sending(self.piece(block, c), self.piece(block, c), sem, self.recv.at[block, c], device).start()

    def wait(self, block, c):
        landed(self.piece(block, c), self.recv.at[block, c])

    def right(self, c):
        self.send(self.at.me, c, self.to_right.at[c], self.at.right)

    def left(self, c):
        self.send(self.at.me, c, self.to_left.at[c], self.at.left)

    def sib(self, c):
        self.send(self.at.me, c, self.to_sib.at[c], self.at.sib)

    def start(self, make):
        make(0)
        self.right(0), self.sib(0)
        make(2)
        self.left(2), self.sib(2)
        make(1)
        self.right(1), self.sib(1)
        make(3)
        self.left(3), self.sib(3)

    def step(self, s):
        at = self.at
        if s // 2 == 1:
            a, b, i, j = at.far, at.far, s - 2, s
            ka, kb = 3, 3
        else:
            a, b, i, j = at.left, at.right, s - s // 4 * 2, (s + 2) % 6 if s < 4 else s - 4
            ka, kb = 1, 2
        self.wait(a, i)
        if s < 2:
            self.send(a, i, self.to_right.at[CHUNKS + s], at.right)
        self.wait(b, j)
        if s < 2:
            self.send(b, j, self.to_left.at[CHUNKS + s], at.left)
        if s == 1:
            self.right(2), self.left(0), self.right(3), self.left(1)
        self.send(a, i, self.to_sib.at[CHUNKS * ka + i], at.sib)
        self.send(b, j, self.to_sib.at[CHUNKS * kb + j], at.sib)
        return i, j

    def left_all(self):
        for sems, count in ((self.to_right, CHUNKS + 2), (self.to_left, CHUNKS + 2), (self.to_sib, 4 * CHUNKS)):
            for c in range(count):
                landed(self.piece(self.at.me, 0), sems.at[c])


def layer(n, x_hbm, gain_a_ref, wq_hbm, wk_hbm, wv_hbm, wo_hbm, gain_m_ref, wg_hbm, wu_hbm, wd_hbm, row_ref, block_ref, y_hbm,
          slots, hid_s, wo_s, wg_s, wu_s, wd_s, run_s, from_s, xh_s, top_s, mix_s,
          recv, to_right, to_left, to_sib, wo_recv, wo_right, wo_left, wo_sib, all_send, all_recv,
          term_send, term_recv, ring_send, ring_recv, local, local_x):
    at = Place(n)
    me = at.me
    rows, d = xh_s.shape
    width = wq_hbm.shape[1]
    half, wide = rows // 2, d // 2
    q_at, k_at, seen_at, got_at = (i * width for i in range(4))
    tall = HEAD + 16

    g = Gather(at, slots, recv, to_right, to_left, to_sib)
    size = g.rows
    x_loads = [pltpu.make_async_copy(x_hbm.at[pl.ds(c * size, size), :], xh_s.at[pl.ds(c * size, size), :], local_x.at[c]) for c in range(CHUNKS)]
    loads = [pltpu.make_async_copy(w, wg_s.at[:, pl.ds(i * width, width)], local.at[i]) for i, w in enumerate((wq_hbm, wk_hbm, wv_hbm))]
    loads += [pltpu.make_async_copy(wo_hbm, wo_s.at[me], local.at[3]), pltpu.make_async_copy(wu_hbm, wu_s, local.at[4])]
    late = [pltpu.make_async_copy(wg_hbm, wg_s, local.at[5]), pltpu.make_async_copy(wd_hbm, wd_s, local.at[6])]
    for c in (0, 2, 1, 3):
        x_loads[c].start()
    for load in loads[:3]:
        load.start()
    barrier = pltpu.get_barrier_semaphore()
    for k in range(1, n):
        pl.semaphore_signal(barrier, inc=1, device_id={"tp": lax.rem(me + k, n)}, device_id_type=MESH)

    def norm(c, gain_ref):
        here = pl.ds(c * size, size)
        slots[me, here, :] = normed(xh_s[here, :], gain_ref[...])

    def first(c):
        x_loads[c].wait()
        norm(c, gain_a_ref)

    first(0)
    first(2)
    pl.semaphore_wait(barrier, n - 1)
    g.start(lambda c: first(c) if c % 2 else None)
    for i in range(4):
        wd_s[i * tall + HEAD : (i + 1) * tall, :] = jnp.ones((tall - HEAD, d), jnp.bfloat16)
    for load in loads[:3]:
        load.wait()
    sign = jnp.where(lax.broadcasted_iota(jnp.int32, (1, HEAD), 1) < HEAD // 2, -1.0, 1.0)

    def value_at(h, b):
        return pl.multiple_of((2 * h + lax.div(b, n // 2)) * tall, 16), pl.multiple_of(lax.rem(b, n // 2) * rows, rows)

    def project(b, c):
        here = pl.ds(pl.multiple_of(c * size, size), size)
        a = slots[b, here, :]
        cr, sr = row_ref[0, here, :], row_ref[1, here, :]
        cb, sb = block_ref[0, pl.ds(b, 1), :], block_ref[1, pl.ds(b, 1), :]
        cos, sin = cr * cb - sr * sb, (sr * cb + cr * sb) * sign
        for w, out in ((0, q_at), (1, k_at)):
            t = dot(a, wg_s[:, w * width : (w + 1) * width]).astype(jnp.bfloat16).astype(jnp.float32)
            for h in range(2):
                one = t[:, h * HEAD : (h + 1) * HEAD]
                turned = one * cos + pltpu.roll(one, HEAD // 2, 1) * sin
                hid_s[b, here, out + h * HEAD : out + (h + 1) * HEAD] = turned.astype(jnp.bfloat16)
        t = dot(a, wg_s[:, 2 * width : 3 * width])
        for h in range(2):
            r, first = value_at(h, b)
            wd_s[pl.ds(r, HEAD), pl.ds(pl.multiple_of(first + c * size, size), size)] = t[:, h * HEAD : (h + 1) * HEAD].T.astype(jnp.bfloat16)

    for c in range(CHUNKS):
        g.wait(at.sib, c)
    lax.fori_loop(0, 2 * CHUNKS, lambda i, _: project(at.at(0, lax.div(i, CHUNKS)), lax.rem(i, CHUNKS)), None)

    def wo_piece(b, c):
        return wo_s.at[b, pl.ds(c * HEAD, HEAD), :]

    def wo_send(b, c, sem, device):
        sending(wo_piece(b, c), wo_piece(b, c), sem, wo_recv.at[b, c], device).start()

    def wo_wait(b, c):
        landed(wo_piece(b, c), wo_recv.at[b, c])

    near = lambda side: n // 2 - 1 + 2 * side
    two = lambda side: 2
    for s in range(6):
        i, j = g.step(s)
        if s == 1:
            loads[3].start()
            loads[4].start()
        if s == 4:
            loads[3].wait()
            wo_send(me, 0, wo_right.at[0], at.right)
            wo_send(me, 1, wo_left.at[1], at.left)
            wo_send(me, 1, wo_right.at[1], at.right)
            wo_send(me, 0, wo_left.at[0], at.left)
            for c in range(2):
                wo_send(me, c, wo_sib.at[c], at.sib)
        off = two if s // 2 == 1 else near
        g.wait(at.at(off(0), 1), i)
        g.wait(at.at(off(1), 1), j)
        lax.fori_loop(0, 4, lambda k, _: project(at.at(off(lax.rem(k, 2)), lax.div(k, 2)), i + lax.rem(k, 2) * (j - i)), None)
    late[0].start()

    e = HEAD**-0.5 * LOG2E

    def attend(key, b, strips, masked):
        pieces = [(h, i) for i in strips for h in range(2)]
        scores = [dot(hid_s[key, :, k_at + h * HEAD : k_at + (h + 1) * HEAD], hid_s[b + i, :, q_at + h * HEAD : q_at + (h + 1) * HEAD], 1, 1)
                  for h, i in pieces]
        weights, keeps = [], []
        for (h, i), s in zip(pieces, scores):
            if i in masked:
                ok = lax.broadcasted_iota(jnp.int32, s.shape, 1) >= lax.broadcasted_iota(jnp.int32, s.shape, 0)
                s = jnp.where(ok, s, HIDDEN)
            r = 2 * i + h
            old = top_s[r : r + 1, :]
            top = jnp.maximum(old, s.max(axis=0, keepdims=True))
            top_s[r : r + 1, :] = top
            weights.append(jnp.exp2((s - top) * e).astype(jnp.bfloat16))
            keeps.append(jnp.exp2((old - top) * e))
        for (h, i), p, keep in zip(pieces, weights, keeps):
            r = 2 * i + h
            row, first = value_at(h, key)
            mix_s[r] = mix_s[r] * keep + dot(wd_s[pl.ds(row, HEAD + 8), pl.ds(first, rows)], p)

    def seen(b):
        return hid_s.at[b, :, pl.ds(seen_at, width)]

    def got(b):
        return hid_s.at[b, :, pl.ds(got_at, width)]

    def share(b):
        sending(seen(b), got(me), all_send.at[b], all_recv.at[me], b).start()

    def turn(t, _):
        b = lax.rem(at.chip + t + 1, n // 2) * 2
        top_s[...] = jnp.full(top_s.shape, NEG, jnp.float32)
        mix_s[...] = jnp.zeros(mix_s.shape, jnp.float32)
        lax.fori_loop(0, b, lambda key, _: attend(key, b, (0, 1), ()), None)
        attend(b, b, (0, 1), (0,))
        attend(b + 1, b, (1,), (1,))
        for i in range(2):
            for h in range(2):
                m = mix_s[2 * i + h]
                o = m[:HEAD] * (1 / m[HEAD : HEAD + 1])
                hid_s[b + i, :, seen_at + h * HEAD : seen_at + (h + 1) * HEAD] = o.T.astype(jnp.bfloat16)

        @pl.when(t == 0)
        def _():
            g.left_all()
            wo_wait(at.left, 0)
            wo_send(at.left, 0, wo_right.at[2], at.right)
            wo_wait(at.right, 1)
            wo_send(at.right, 1, wo_left.at[2], at.left)
            wo_send(at.left, 0, wo_sib.at[2], at.sib)
            wo_send(at.right, 1, wo_sib.at[5], at.sib)

        @pl.when(t == 1)
        def _():
            wo_wait(at.left, 1)
            wo_send(at.left, 1, wo_sib.at[3], at.sib)
            wo_wait(at.right, 0)
            wo_send(at.right, 0, wo_sib.at[4], at.sib)

        @pl.when(t < n // 2 - 1)
        def _():
            share(b)
            share(b + 1)

    lax.fori_loop(0, n // 2, turn, None)
    late[1].start()
    share(at.sib)
    for c in range(2):
        wo_wait(at.far, c)
        wo_send(at.far, c, wo_sib.at[6 + c], at.sib)
    got(me)[...] = seen(me)[...]
    for off in range(n // 2):
        for c in range(2):
            wo_wait(at.at(off, 1), c)
    for k in range(3):
        landed(wo_piece(me, 0), wo_right.at[k])
        landed(wo_piece(me, 0), wo_left.at[k])
    for k in range(8):
        landed(wo_piece(me, 0), wo_sib.at[k])
    for k in range(1, n):
        b = lax.rem(me + k, n)
        landed(got(b), all_recv.at[b])
    tile = 512

    def finish(c):
        here = pl.ds(c * size, size)

        def out(t, _):
            cols = pl.ds(pl.multiple_of(t * tile, tile), tile)
            total = dot(hid_s[0, here, got_at : got_at + width], wo_s[0, :, cols])
            for b in range(1, n):
                total += dot(hid_s[b, here, got_at : got_at + width], wo_s[b, :, cols])
            xh_s[here, cols] = (xh_s[here, cols].astype(jnp.float32) + total).astype(jnp.bfloat16)

        lax.fori_loop(0, d // tile, out, None)
        norm(c, gain_m_ref)

    g.start(finish)

    for k in range(1, n):
        b = lax.rem(me + k, n)
        landed(seen(b), all_send.at[b])
    loads[4].wait()
    late[0].wait()
    cut = 256
    cuts = hid_s.shape[2] // cut

    def hidden(b, part, t):
        here = pl.ds(pl.multiple_of(part * half, half), half)
        cols = pl.ds(pl.multiple_of(t * cut, cut), cut)
        a = slots[b, here, :]
        gate, up = dot(a, wg_s[:, cols]), dot(a, wu_s[:, cols])
        hid_s[b, here, cols] = (jax.nn.silu(gate) * up).astype(jnp.bfloat16)

    def four(off, part):
        def one(i, _):
            k, t = lax.div(i, cuts), lax.rem(i, cuts)
            side = lax.rem(k, 2)
            hidden(at.at(off(side), lax.div(k, 2)), part(side), t)
        lax.fori_loop(0, 4 * cuts, one, None)

    for c in range(CHUNKS):
        g.wait(at.sib, c)
    four(lambda side: 0, lambda side: side)

    def piece(ref, index, part, c):
        return ref.at[(*index, pl.ds(pl.multiple_of(part * half, half), half), pl.ds(pl.multiple_of(c * wide, wide), wide))]

    def term(b, part, c):
        rows_ = pl.ds(pl.multiple_of(part * half, half), half)
        return dot(hid_s[b, rows_, :], wd_s[:, pl.ds(pl.multiple_of(c * wide, wide), wide)])

    def give(k, off, part):
        def one(index, _):
            c, i = lax.div(index, 2), lax.rem(index, 2)
            other = at.at(off(i), 1)
            source = piece(slots, (other,), part(i), c)
            source[...] = term(other, part(i), c).astype(jnp.bfloat16)
            sending(source, piece(wo_s, (2 * k + i,), 0, c), term_send.at[k, i, c], term_recv.at[k, i, c], at.sib).start()

        lax.fori_loop(0, 4, one, None)

    def chips_term(k, off, part, i, c):
        mine = term(at.at(off), part, c)
        target = piece(wo_s, (2 * k + i,), 0, c)
        landed(target, term_recv.at[k, i, c])
        return mine + target[...].astype(jnp.float32)

    def group(k, off, part, stage, extra=False):
        give(k, off, part)

        def one(index, _):
            c, i = lax.div(index, 2), lax.rem(index, 2)
            total = chips_term(k, off(i), part(i), i, c)
            if extra:
                came = piece(run_s, (i,), 0, c)
                landed(came, ring_recv.at[1, i, c])
                total += came[...].astype(jnp.float32)
            source = piece(slots, (stage(i),), part(i), c)
            source[...] = total.astype(jnp.bfloat16)
            target = piece(run_s, (i,), 0, c) if k == 1 else piece(from_s, (i,), part(i), c)
            sending(source, target, ring_send.at[k, i, c], ring_recv.at[k, i, c], lax.rem(me + 2 + (n - 4) * i, n)).start()

        lax.fori_loop(0, 4, one, None)

    turned = lambda i: 1 + (n // 2 - 2) * i

    def pair(s):
        off = two if s // 2 == 1 else near
        i, j = ends[s]
        for c in (i - 1, i):
            g.wait(at.at(off(0), 1), c)
        for c in (j - 1, j):
            g.wait(at.at(off(1), 1), c)
        first, last = i // 2, j // 2
        four(off, lambda side: first + side * (last - first))

    ends = {}
    for s in range(6):
        ends[s] = g.step(s)
        if s == 1:
            pair(1)
            late[1].wait()
        elif s == 2:
            group(0, turned, lambda i: 1 - i, lambda i: at.sib)
        elif s == 3:
            pair(3)
        elif s == 4:
            g_far = lambda i: at.far
            for c in range(CHUNKS):
                landed(g.piece(me, 0), to_sib.at[3 * CHUNKS + c])
            group(1, two, lambda i: i, g_far)
        elif s == 5:
            pair(5)
    for sems, count in ((to_right, CHUNKS + 2), (to_left, CHUNKS + 2), (to_sib, 3 * CHUNKS)):
        for c in range(count):
            landed(g.piece(me, 0), sems.at[c])
    group(2, turned, lambda i: i, lambda i: at.at(turned(i)), extra=True)
    for i in range(2):
        for c in range(2):
            landed(piece(slots, (me,), 0, 0), ring_send.at[0, i, c])
    give(3, lambda i: 0, lambda i: i)

    def last(index, _):
        c, i = lax.div(index, 2), lax.rem(index, 2)
        total = chips_term(3, 0, i, i, c)
        here = piece(xh_s, (), i, c)
        total += here[...].astype(jnp.float32)
        for side in range(2):
            came = piece(from_s, (side,), i, c)
            kind = 2 * (1 - i) if side == 0 else 2 * i
            landed(came, ring_recv.at[kind, side, c])
            total += came[...].astype(jnp.float32)
        source = piece(slots, (me,), i, c)
        source[...] = total.astype(jnp.bfloat16)
        pltpu.make_async_copy(source, piece(y_hbm, (), i, c), local_x.at[index]).start()

    lax.fori_loop(0, 4, last, None)
    for i in range(2):
        for c in range(2):
            for k in range(4):
                landed(piece(slots, (me,), 0, 0), term_send.at[k, i, c])
            for k in range(1, 3):
                landed(piece(slots, (me,), 0, 0), ring_send.at[k, i, c])
            landed(piece(slots, (me,), 0, 0), local_x.at[2 * c + i])


def tables(rows, n):
    freq = float(THETA) ** (-np.arange(HEAD // 2) / (HEAD // 2))

    def both(place):
        angle = np.tile(place[:, None] * freq, (1, 2))
        return jnp.asarray(np.stack([np.cos(angle), np.sin(angle)]).astype(np.float32))

    return both(np.arange(rows)), both(np.arange(n) * rows)


def solution(mesh):
    n = mesh.shape["tp"]
    vmem, hbm = pl.BlockSpec(memory_space=pltpu.VMEM), pl.BlockSpec(memory_space=pl.ANY)
    dma = pltpu.SemaphoreType.DMA
    bf16 = jnp.bfloat16

    def step(x, gain_a, wq, wk, wv, wo, gain_m, w_gate, w_up, w_down):
        rows, d = x.shape
        width, units = wq.shape[1], w_gate.shape[1]
        row_table, block_table = tables(rows, n)
        return pl.pallas_call(
            functools.partial(layer, n),
            name="layer",
            out_shape=jax.ShapeDtypeStruct((rows, d), bf16),
            in_specs=[hbm, vmem, hbm, hbm, hbm, hbm, vmem, hbm, hbm, hbm, vmem, vmem],
            out_specs=hbm,
            scratch_shapes=[
                pltpu.VMEM((n, rows, d), bf16),
                pltpu.VMEM((n, rows, units), bf16),
                pltpu.VMEM((n, width, d), bf16),
                pltpu.VMEM((d, units), bf16),
                pltpu.VMEM((d, units), bf16),
                pltpu.VMEM((units, d), bf16),
                pltpu.VMEM((2, rows // 2, d), bf16),
                pltpu.VMEM((2, rows, d), bf16),
                pltpu.VMEM((rows, d), bf16),
                pltpu.VMEM((4, rows), jnp.float32),
                pltpu.VMEM((4, HEAD + 8, rows), jnp.float32),
                dma((n, CHUNKS)), dma((CHUNKS + 2,)), dma((CHUNKS + 2,)), dma((4 * CHUNKS,)),
                dma((n, 2)), dma((3,)), dma((3,)), dma((8,)), dma((n,)), dma((n,)),
                dma((4, 2, 2)), dma((4, 2, 2)), dma((3, 2, 2)), dma((3, 2, 2)), dma((7,)), dma((CHUNKS,)),
            ],
            compiler_params=pltpu.CompilerParams(collective_id=0, has_side_effects=True, vmem_limit_bytes=LIMIT),
        )(x, gain_a, wq, wk, wv, wo, gain_m, w_gate, w_up, w_down, row_table, block_table)

    tokens, columns, rows_of = P(("dp", "tp"), None), P(None, "tp"), P("tp", None)
    return jax.shard_map(
        step,
        mesh=mesh,
        in_specs=(tokens, P(None), columns, columns, columns, rows_of, P(None), columns, columns, rows_of),
        out_specs=tokens,
        check_vma=False,
    )
```

```python
import functools

import jax
import jax.numpy as jnp
import numpy as np
from jax import lax
from jax.experimental import pallas as pl
from jax.experimental.pallas import tpu as pltpu
from jax.sharding import PartitionSpec as P

MESH = pl.DeviceIdType.MESH
HEAD = 128
THETA = 10000
NEG = -1e30
HIDDEN = 2 * NEG
LOG2E = 1.4426950408889634
CHUNKS = 4
LIMIT = 67_000_000


def normed(x, gain):
    wide = x.astype(jnp.float32)
    scale = lax.rsqrt(jnp.mean(wide * wide, -1, keepdims=True) + 1e-6)
    return (wide * scale * gain.astype(jnp.float32)).astype(jnp.bfloat16)


def dot(a, b, ca=1, cb=0):
    return lax.dot_general(a, b, (((ca,), (cb,)), ((), ())), preferred_element_type=jnp.float32)


def sending(src, dst, send_sem, recv_sem, device):
    return pltpu.make_async_remote_copy(
        src_ref=src, dst_ref=dst, send_sem=send_sem, recv_sem=recv_sem, device_id={"tp": device}, device_id_type=MESH
    )


def landed(dst, sem):
    pltpu.make_async_copy(dst, dst, sem).wait()


class Place:
    def __init__(self, n):
        self.n = n
        self.me = lax.axis_index("tp")
        self.core = lax.rem(self.me, 2)
        self.chip = lax.div(self.me, 2)
        self.sib = self.me + 1 - 2 * self.core
        self.right, self.left, self.far = (lax.rem(self.me + 2 * k, n) for k in (1, n // 2 - 1, 2))

    def at(self, off, other=0):
        return lax.rem(self.chip + off, self.n // 2) * 2 + lax.rem(self.core + other, 2)


class Gather:
    def __init__(self, at, slots, recv, to_right, to_left, to_sib):
        self.at, self.slots, self.recv, self.to_right, self.to_left, self.to_sib = at, slots, recv, to_right, to_left, to_sib
        self.rows = slots.shape[1] // CHUNKS

    def piece(self, block, c):
        return self.slots.at[block, pl.ds(c * self.rows, self.rows), :]

    def send(self, block, c, sem, device):
        sending(self.piece(block, c), self.piece(block, c), sem, self.recv.at[block, c], device).start()

    def wait(self, block, c):
        landed(self.piece(block, c), self.recv.at[block, c])

    def right(self, c):
        self.send(self.at.me, c, self.to_right.at[c], self.at.right)

    def left(self, c):
        self.send(self.at.me, c, self.to_left.at[c], self.at.left)

    def sib(self, c):
        self.send(self.at.me, c, self.to_sib.at[c], self.at.sib)

    def start(self, make):
        make(0)
        self.right(0), self.sib(0)
        make(2)
        self.left(2), self.sib(2)
        make(1)
        self.right(1), self.sib(1)
        make(3)
        self.left(3), self.sib(3)

    def step(self, s):
        at = self.at
        if s // 2 == 1:
            a, b, i, j = at.far, at.far, s - 2, s
            ka, kb = 3, 3
        else:
            a, b, i, j = at.left, at.right, s - s // 4 * 2, (s + 2) % 6 if s < 4 else s - 4
            ka, kb = 1, 2
        self.wait(a, i)
        if s < 2:
            self.send(a, i, self.to_right.at[CHUNKS + s], at.right)
        self.wait(b, j)
        if s < 2:
            self.send(b, j, self.to_left.at[CHUNKS + s], at.left)
        if s == 1:
            self.right(2), self.left(0), self.right(3), self.left(1)
        self.send(a, i, self.to_sib.at[CHUNKS * ka + i], at.sib)
        self.send(b, j, self.to_sib.at[CHUNKS * kb + j], at.sib)
        return i, j

    def left_all(self):
        for sems, count in ((self.to_right, CHUNKS + 2), (self.to_left, CHUNKS + 2), (self.to_sib, 4 * CHUNKS)):
            for c in range(count):
                landed(self.piece(self.at.me, 0), sems.at[c])


def layer(n, x_hbm, gain_a_ref, wq_hbm, wk_hbm, wv_hbm, wo_hbm, gain_m_ref, wg_hbm, wu_hbm, wd_hbm, row_ref, block_ref, y_hbm,
          slots, hid_s, wo_s, wg_s, wu_s, wd_s, run_s, from_s, xh_s, top_s, mix_s,
          recv, to_right, to_left, to_sib, wo_recv, wo_right, wo_left, wo_over, wo_sib, all_send, all_recv,
          term_send, term_recv, ring_send, ring_recv, local, local_x):
    at = Place(n)
    me = at.me
    rows, d = xh_s.shape
    width = wq_hbm.shape[1]
    half, wide = rows // 2, d // 2
    q_at, k_at, seen_at, got_at = (i * width for i in range(4))
    tall = HEAD + 16

    g = Gather(at, slots, recv, to_right, to_left, to_sib)
    size = g.rows
    x_loads = [pltpu.make_async_copy(x_hbm.at[pl.ds(c * size, size), :], xh_s.at[pl.ds(c * size, size), :], local_x.at[c]) for c in range(CHUNKS)]
    loads = [pltpu.make_async_copy(w, wg_s.at[:, pl.ds(i * width, width)], local.at[i]) for i, w in enumerate((wq_hbm, wk_hbm, wv_hbm))]
    loads += [pltpu.make_async_copy(wo_hbm, wo_s.at[me], local.at[3]), pltpu.make_async_copy(wu_hbm, wu_s, local.at[4])]
    late = [pltpu.make_async_copy(wg_hbm, wg_s, local.at[5]), pltpu.make_async_copy(wd_hbm, wd_s, local.at[6])]
    for c in (0, 2, 1, 3):
        x_loads[c].start()
    for load in loads[:3]:
        load.start()
    barrier = pltpu.get_barrier_semaphore()
    for k in range(1, n):
        pl.semaphore_signal(barrier, inc=1, device_id={"tp": lax.rem(me + k, n)}, device_id_type=MESH)
    odd = lax.rem(lax.axis_index("dp"), 2)
    twin = {"dp": lax.axis_index("dp") + 1 - 2 * odd, "tp": me}
    pl.semaphore_signal(barrier, inc=1, device_id=twin, device_id_type=MESH)

    def norm(c, gain_ref):
        here = pl.ds(c * size, size)
        slots[me, here, :] = normed(xh_s[here, :], gain_ref[...])

    def first(c):
        x_loads[c].wait()
        norm(c, gain_a_ref)

    first(0)
    first(2)
    pl.semaphore_wait(barrier, n)
    g.start(lambda c: first(c) if c % 2 else None)
    for i in range(4):
        wd_s[i * tall + HEAD : (i + 1) * tall, :] = jnp.ones((tall - HEAD, d), jnp.bfloat16)
    for load in loads[:3]:
        load.wait()
    sign = jnp.where(lax.broadcasted_iota(jnp.int32, (1, HEAD), 1) < HEAD // 2, -1.0, 1.0)

    def value_at(h, b):
        return pl.multiple_of((2 * h + lax.div(b, n // 2)) * tall, 16), pl.multiple_of(lax.rem(b, n // 2) * rows, rows)

    def project(b, c):
        here = pl.ds(pl.multiple_of(c * size, size), size)
        a = slots[b, here, :]
        cr, sr = row_ref[0, here, :], row_ref[1, here, :]
        cb, sb = block_ref[0, pl.ds(b, 1), :], block_ref[1, pl.ds(b, 1), :]
        cos, sin = cr * cb - sr * sb, (sr * cb + cr * sb) * sign
        for w, out in ((0, q_at), (1, k_at)):
            t = dot(a, wg_s[:, w * width : (w + 1) * width]).astype(jnp.bfloat16).astype(jnp.float32)
            for h in range(2):
                one = t[:, h * HEAD : (h + 1) * HEAD]
                turned = one * cos + pltpu.roll(one, HEAD // 2, 1) * sin
                hid_s[b, here, out + h * HEAD : out + (h + 1) * HEAD] = turned.astype(jnp.bfloat16)
        t = dot(a, wg_s[:, 2 * width : 3 * width])
        for h in range(2):
            r, first = value_at(h, b)
            wd_s[pl.ds(r, HEAD), pl.ds(pl.multiple_of(first + c * size, size), size)] = t[:, h * HEAD : (h + 1) * HEAD].T.astype(jnp.bfloat16)

    for c in range(CHUNKS):
        g.wait(at.sib, c)
    lax.fori_loop(0, 2 * CHUNKS, lambda i, _: project(at.at(0, lax.div(i, CHUNKS)), lax.rem(i, CHUNKS)), None)

    lone, run = 3 * width // 16, 5 * width // 16

    def wo_rows(b, kind):
        if kind < 2:
            start, count = (lone * odd, width - run - lone * odd)[kind], run
        else:
            who = odd if kind > 3 else 1 - odd
            start, count = (run * who, width - lone - run * who)[kind % 2], lone
        return wo_s.at[b, pl.ds(pl.multiple_of(start, 16), count), :]

    def wo_send(b, kind, sem, device):
        sending(wo_rows(b, kind), wo_rows(b, kind), sem, wo_recv.at[b, kind], device).start()

    def wo_wait(b, kind):
        landed(wo_rows(b, kind), wo_recv.at[b, kind])

    def wo_start():
        wo_send(me, 0, wo_right.at[0], at.right)
        wo_send(me, 1, wo_left.at[0], at.left)
        wo_send(me, 1, wo_right.at[1], at.right)
        wo_send(me, 0, wo_left.at[1], at.left)
        sending(wo_s.at[me], wo_s.at[me], wo_sib.at[0, 0], wo_recv.at[me, 0], at.sib).start()

    def wo_cross(k, kind):
        b = (at.left, at.right, at.far)[k]
        piece = wo_rows(b, 4 + kind)
        pltpu.make_async_remote_copy(
            src_ref=piece, dst_ref=piece, send_sem=wo_over.at[k, kind], recv_sem=wo_recv.at[b, 2 + kind], device_id=twin, device_id_type=MESH
        ).start()
        wo_send(b, kind, wo_sib.at[1 + k, kind], at.sib)

    def errands(u):
        @pl.when(u == 3)
        def _():
            wo_wait(at.left, 0)
            wo_send(at.left, 0, wo_right.at[2], at.right)
            wo_wait(at.right, 1)
            wo_send(at.right, 1, wo_left.at[2], at.left)
            wo_cross(0, 0)
            wo_cross(1, 1)

        @pl.when(u == 10)
        def _():
            wo_wait(at.left, 1)
            wo_cross(0, 1)
            wo_wait(at.right, 0)
            wo_cross(1, 0)

        @pl.when(u == 18)
        def _():
            for kind in range(2):
                wo_wait(at.far, kind)
                wo_cross(2, kind)

    e = HEAD**-0.5 * LOG2E
    part = rows // 2
    pieces = [(h, i) for h in range(2) for i in range(2)]

    def attend(key, b, slot, masked=False):
        scores = [dot(hid_s[key, :, k_at + h * HEAD : k_at + (h + 1) * HEAD],
                      hid_s[b, i * part : (i + 1) * part, q_at + h * HEAD : q_at + (h + 1) * HEAD], 1, 1) for h, i in pieces]
        weights, keeps = [], []
        for r, ((h, i), s) in enumerate(zip(pieces, scores)):
            if masked:
                ok = lax.broadcasted_iota(jnp.int32, s.shape, 1) + i * part >= lax.broadcasted_iota(jnp.int32, s.shape, 0)
                s = jnp.where(ok, s, HIDDEN)
            old = top_s[slot, r : r + 1, :]
            top = jnp.maximum(old, s.max(axis=0, keepdims=True))
            top_s[slot, r : r + 1, :] = top
            weights.append(jnp.exp2((s - top) * e).astype(jnp.bfloat16))
            keeps.append(jnp.exp2((old - top) * e))
        for r, ((h, i), p, keep) in enumerate(zip(pieces, weights, keeps)):
            row, first = value_at(h, key)
            mix_s[slot, r] = mix_s[slot, r] * keep + dot(wd_s[pl.ds(row, HEAD + 8), pl.ds(first, rows)], p)

    def clear(slot):
        top_s[slot] = jnp.full(top_s.shape[1:], NEG, jnp.float32)
        mix_s[slot] = jnp.zeros(mix_s.shape[1:], jnp.float32)

    def seen(b):
        return hid_s.at[b, :, pl.ds(seen_at, width)]

    def got(b):
        return hid_s.at[b, :, pl.ds(got_at, width)]

    def share(b):
        sending(seen(b), got(me), all_send.at[b], all_recv.at[me], b).start()

    def done(b, slot):
        for r, (h, i) in enumerate(pieces):
            m = mix_s[slot, r]
            o = m[:HEAD] * (1 / m[HEAD : HEAD + 1])
            hid_s[b, i * part : (i + 1) * part, seen_at + h * HEAD : seen_at + (h + 1) * HEAD] = o.T.astype(jnp.bfloat16)

    par = lax.rem(at.chip, 2)

    def key_of(m, p):
        return 2 * p + lax.div(m, 2) * 4 + lax.rem(m, 2)

    def early(i, _):
        b = key_of(i, par)
        clear(i)
        lax.fori_loop(0, i, lambda m, _: attend(key_of(m, par), b, i), None)
        attend(b, b, i, True)

    def sides(j, u):
        b = at.at(1 + (n // 2 - 2) * lax.rem(j, 2)) - at.core + lax.div(j, 2)
        clear(4)

        def one(m, _):
            attend(m, b, 4)
            errands(u + m)

        lax.fori_loop(0, b, one, None)
        attend(b, b, 4, True)
        errands(u + b)
        done(b, 4)
        share(b)
        return u + b + 1

    def across(j, u):
        chip = lax.rem(at.chip + 2 - lax.div(j, 2) * 2, n // 2)
        b = 2 * chip + lax.rem(j, 2)
        count = 2 * lax.div(chip + 1, 2)
        slot = 2 * lax.div(chip, 2) + lax.rem(j, 2)

        def one(m, _):
            attend(key_of(m, 1 - par), b, slot)
            errands(u + m)

        lax.fori_loop(0, count, one, None)
        done(b, slot)

        @pl.when(j < 2)
        def _():
            share(b)

        return u + count

    near = lambda side: n // 2 - 1 + 2 * side
    two = lambda side: 2
    for s in range(6):
        i, j = g.step(s)
        if s == 1:
            loads[3].start()
            loads[4].start()
        if s == 4:
            loads[3].wait()
            wo_start()
        off = two if s // 2 == 1 else near
        g.wait(at.at(off(0), 1), i)
        g.wait(at.at(off(1), 1), j)
        lax.fori_loop(0, 4, lambda k, _: project(at.at(off(lax.rem(k, 2)), lax.div(k, 2)), i + lax.rem(k, 2) * (j - i)), None)
        if s == 3:
            lax.fori_loop(0, 4, early, None)
    late[0].start()
    g.left_all()
    lax.fori_loop(0, 4, across, lax.fori_loop(0, 4, sides, 0))
    late[1].start()

    share(at.sib)
    for k, kind in ((0, 0), (1, 1), (0, 1), (1, 0), (2, 0), (2, 1)):
        b = (at.left, at.right, at.far)[k]
        wo_wait(b, 2 + kind)
        wo_send(b, 2 + kind, wo_sib.at[1 + k, 2 + kind], at.sib)
    got(me)[...] = seen(me)[...]
    landed(wo_s.at[at.sib], wo_recv.at[at.sib, 0])
    for off in range(1, n // 2):
        for kind in range(4):
            wo_wait(at.at(off, 1), kind)
    for k in range(3):
        landed(wo_rows(me, 0), wo_right.at[k])
        landed(wo_rows(me, 0), wo_left.at[k])
        for kind in range(2):
            landed(wo_rows(me, 2), wo_over.at[k, kind])
            landed(wo_rows(me, 0), wo_sib.at[1 + k, kind])
            landed(wo_rows(me, 2), wo_sib.at[1 + k, 2 + kind])
    landed(wo_s.at[me], wo_sib.at[0, 0])
    for k in range(1, n):
        b = lax.rem(me + k, n)
        landed(got(b), all_recv.at[b])
    tile = 512

    def finish(c):
        here = pl.ds(c * size, size)

        def out(t, _):
            cols = pl.ds(pl.multiple_of(t * tile, tile), tile)
            total = dot(hid_s[0, here, got_at : got_at + width], wo_s[0, :, cols])
            for b in range(1, n):
                total += dot(hid_s[b, here, got_at : got_at + width], wo_s[b, :, cols])
            xh_s[here, cols] = (xh_s[here, cols].astype(jnp.float32) + total).astype(jnp.bfloat16)

        lax.fori_loop(0, d // tile, out, None)
        norm(c, gain_m_ref)

    g.start(finish)

    for k in range(1, n):
        b = lax.rem(me + k, n)
        landed(seen(b), all_send.at[b])
    loads[4].wait()
    late[0].wait()
    cut = 256
    cuts = hid_s.shape[2] // cut

    def hidden(b, part, t):
        here = pl.ds(pl.multiple_of(part * half, half), half)
        cols = pl.ds(pl.multiple_of(t * cut, cut), cut)
        a = slots[b, here, :]
        gate, up = dot(a, wg_s[:, cols]), dot(a, wu_s[:, cols])
        hid_s[b, here, cols] = (jax.nn.silu(gate) * up).astype(jnp.bfloat16)

    def four(off, part):
        def one(i, _):
            k, t = lax.div(i, cuts), lax.rem(i, cuts)
            side = lax.rem(k, 2)
            hidden(at.at(off(side), lax.div(k, 2)), part(side), t)
        lax.fori_loop(0, 4 * cuts, one, None)

    for c in range(CHUNKS):
        g.wait(at.sib, c)
    four(lambda side: 0, lambda side: side)

    def piece(ref, index, part, c):
        return ref.at[(*index, pl.ds(pl.multiple_of(part * half, half), half), pl.ds(pl.multiple_of(c * wide, wide), wide))]

    def term(b, part, c):
        rows_ = pl.ds(pl.multiple_of(part * half, half), half)
        return dot(hid_s[b, rows_, :], wd_s[:, pl.ds(pl.multiple_of(c * wide, wide), wide)])

    def give(k, off, part):
        def one(index, _):
            c, i = lax.div(index, 2), lax.rem(index, 2)
            other = at.at(off(i), 1)
            source = piece(slots, (other,), part(i), c)
            source[...] = term(other, part(i), c).astype(jnp.bfloat16)
            sending(source, piece(wo_s, (2 * k + i,), 0, c), term_send.at[k, i, c], term_recv.at[k, i, c], at.sib).start()

        lax.fori_loop(0, 4, one, None)

    def chips_term(k, off, part, i, c):
        mine = term(at.at(off), part, c)
        target = piece(wo_s, (2 * k + i,), 0, c)
        landed(target, term_recv.at[k, i, c])
        return mine + target[...].astype(jnp.float32)

    def group(k, off, part, stage, extra=False):
        give(k, off, part)

        def one(index, _):
            c, i = lax.div(index, 2), lax.rem(index, 2)
            total = chips_term(k, off(i), part(i), i, c)
            if extra:
                came = piece(run_s, (i,), 0, c)
                landed(came, ring_recv.at[1, i, c])
                total += came[...].astype(jnp.float32)
            source = piece(slots, (stage(i),), part(i), c)
            source[...] = total.astype(jnp.bfloat16)
            target = piece(run_s, (i,), 0, c) if k == 1 else piece(from_s, (i,), part(i), c)
            sending(source, target, ring_send.at[k, i, c], ring_recv.at[k, i, c], lax.rem(me + 2 + (n - 4) * i, n)).start()

        lax.fori_loop(0, 4, one, None)

    turned = lambda i: 1 + (n // 2 - 2) * i

    def pair(s):
        off = two if s // 2 == 1 else near
        i, j = ends[s]
        for c in (i - 1, i):
            g.wait(at.at(off(0), 1), c)
        for c in (j - 1, j):
            g.wait(at.at(off(1), 1), c)
        first, last = i // 2, j // 2
        four(off, lambda side: first + side * (last - first))

    ends = {}
    for s in range(6):
        ends[s] = g.step(s)
        if s == 1:
            pair(1)
            late[1].wait()
        elif s == 2:
            group(0, turned, lambda i: 1 - i, lambda i: at.sib)
        elif s == 3:
            pair(3)
        elif s == 4:
            g_far = lambda i: at.far
            for c in range(CHUNKS):
                landed(g.piece(me, 0), to_sib.at[3 * CHUNKS + c])
            group(1, two, lambda i: i, g_far)
        elif s == 5:
            pair(5)
    for sems, count in ((to_right, CHUNKS + 2), (to_left, CHUNKS + 2), (to_sib, 3 * CHUNKS)):
        for c in range(count):
            landed(g.piece(me, 0), sems.at[c])
    group(2, turned, lambda i: i, lambda i: at.at(turned(i)), extra=True)
    for i in range(2):
        for c in range(2):
            landed(piece(slots, (me,), 0, 0), ring_send.at[0, i, c])
    give(3, lambda i: 0, lambda i: i)

    def last(c, _):
        totals = [chips_term(3, 0, i, i, c) + piece(xh_s, (), i, c)[...].astype(jnp.float32) for i in range(2)]
        for i in range(2):
            total = totals[i]
            for side in range(2):
                came = piece(from_s, (side,), i, c)
                kind = 2 * (1 - i) if side == 0 else 2 * i
                landed(came, ring_recv.at[kind, side, c])
                total += came[...].astype(jnp.float32)
            source = piece(slots, (me,), i, c)
            source[...] = total.astype(jnp.bfloat16)
            pltpu.make_async_copy(source, piece(y_hbm, (), i, c), local_x.at[2 * c + i]).start()

    lax.fori_loop(0, 2, last, None)
    for i in range(2):
        for c in range(2):
            for k in range(4):
                landed(piece(slots, (me,), 0, 0), term_send.at[k, i, c])
            for k in range(1, 3):
                landed(piece(slots, (me,), 0, 0), ring_send.at[k, i, c])
            landed(piece(slots, (me,), 0, 0), local_x.at[2 * c + i])


def tables(rows, n):
    freq = float(THETA) ** (-np.arange(HEAD // 2) / (HEAD // 2))

    def both(place):
        angle = np.tile(place[:, None] * freq, (1, 2))
        return jnp.asarray(np.stack([np.cos(angle), np.sin(angle)]).astype(np.float32))

    return both(np.arange(rows)), both(np.arange(n) * rows)


def solution(mesh):
    n = mesh.shape["tp"]
    vmem, hbm = pl.BlockSpec(memory_space=pltpu.VMEM), pl.BlockSpec(memory_space=pl.ANY)
    dma = pltpu.SemaphoreType.DMA
    bf16 = jnp.bfloat16

    def step(x, gain_a, wq, wk, wv, wo, gain_m, w_gate, w_up, w_down):
        rows, d = x.shape
        width, units = wq.shape[1], w_gate.shape[1]
        row_table, block_table = tables(rows, n)
        return pl.pallas_call(
            functools.partial(layer, n),
            name="layer",
            out_shape=jax.ShapeDtypeStruct((rows, d), bf16),
            in_specs=[hbm, vmem, hbm, hbm, hbm, hbm, vmem, hbm, hbm, hbm, vmem, vmem],
            out_specs=hbm,
            scratch_shapes=[
                pltpu.VMEM((n, rows, d), bf16),
                pltpu.VMEM((n, rows, units), bf16),
                pltpu.VMEM((n, width, d), bf16),
                pltpu.VMEM((d, units), bf16),
                pltpu.VMEM((d, units), bf16),
                pltpu.VMEM((units, d), bf16),
                pltpu.VMEM((2, rows // 2, d), bf16),
                pltpu.VMEM((2, rows, d), bf16),
                pltpu.VMEM((rows, d), bf16),
                pltpu.VMEM((5, 4, rows // 2), jnp.float32),
                pltpu.VMEM((5, 4, HEAD + 8, rows // 2), jnp.float32),
                dma((n, CHUNKS)), dma((CHUNKS + 2,)), dma((CHUNKS + 2,)), dma((4 * CHUNKS,)),
                dma((n, 4)), dma((3,)), dma((3,)), dma((3, 2)), dma((4, 4)), dma((n,)), dma((n,)),
                dma((4, 2, 2)), dma((4, 2, 2)), dma((3, 2, 2)), dma((3, 2, 2)), dma((7,)), dma((CHUNKS,)),
            ],
            compiler_params=pltpu.CompilerParams(collective_id=0, has_side_effects=True, vmem_limit_bytes=LIMIT),
        )(x, gain_a, wq, wk, wv, wo, gain_m, w_gate, w_up, w_down, row_table, block_table)

    tokens, columns, rows_of = P(("dp", "tp"), None), P(None, "tp"), P("tp", None)
    return jax.shard_map(
        step,
        mesh=mesh,
        in_specs=(tokens, P(None), columns, columns, columns, rows_of, P(None), columns, columns, rows_of),
        out_specs=tokens,
        check_vma=False,
    )
```

```python
import functools

import jax
import jax.numpy as jnp
import numpy as np
from jax import lax
from jax.experimental import pallas as pl
from jax.experimental.pallas import tpu as pltpu
from jax.sharding import PartitionSpec as P

MESH = pl.DeviceIdType.MESH
HEAD = 128
THETA = 10000
NEG = -1e30
HIDDEN = 2 * NEG
LOG2E = 1.4426950408889634
CHUNKS = 4
LIMIT = 67_000_000


def normed(x, gain):
    wide = x.astype(jnp.float32)
    scale = lax.rsqrt(jnp.mean(wide * wide, -1, keepdims=True) + 1e-6)
    return (wide * scale * gain.astype(jnp.float32)).astype(jnp.bfloat16)


def dot(a, b, ca=1, cb=0):
    return lax.dot_general(a, b, (((ca,), (cb,)), ((), ())), preferred_element_type=jnp.float32)


def sending(src, dst, send_sem, recv_sem, device):
    return pltpu.make_async_remote_copy(
        src_ref=src, dst_ref=dst, send_sem=send_sem, recv_sem=recv_sem, device_id={"tp": device}, device_id_type=MESH
    )


def landed(dst, sem):
    pltpu.make_async_copy(dst, dst, sem).wait()


class Place:
    def __init__(self, n):
        self.n = n
        self.me = lax.axis_index("tp")
        self.core = lax.rem(self.me, 2)
        self.chip = lax.div(self.me, 2)
        self.sib = self.me + 1 - 2 * self.core
        self.right, self.left, self.far = (lax.rem(self.me + 2 * k, n) for k in (1, n // 2 - 1, 2))

    def at(self, off, other=0):
        return lax.rem(self.chip + off, self.n // 2) * 2 + lax.rem(self.core + other, 2)


class Gather:
    def __init__(self, at, slots, recv, to_right, to_left, to_sib):
        self.at, self.slots, self.recv, self.to_right, self.to_left, self.to_sib = at, slots, recv, to_right, to_left, to_sib
        self.rows = slots.shape[1] // CHUNKS

    def piece(self, block, c):
        return self.slots.at[block, pl.ds(c * self.rows, self.rows), :]

    def send(self, block, c, sem, device):
        sending(self.piece(block, c), self.piece(block, c), sem, self.recv.at[block, c], device).start()

    def wait(self, block, c):
        landed(self.piece(block, c), self.recv.at[block, c])

    def right(self, c):
        self.send(self.at.me, c, self.to_right.at[c], self.at.right)

    def left(self, c):
        self.send(self.at.me, c, self.to_left.at[c], self.at.left)

    def sib(self, c):
        self.send(self.at.me, c, self.to_sib.at[c], self.at.sib)

    def start(self, make):
        make(0)
        self.right(0), self.sib(0)
        make(2)
        self.left(2), self.sib(2)
        make(1)
        self.right(1), self.sib(1)
        make(3)
        self.left(3), self.sib(3)

    def step(self, s, between=lambda: None):
        at = self.at
        if s // 2 == 1:
            a, b, i, j = at.far, at.far, s - 2, s
            ka, kb = 3, 3
        else:
            a, b, i, j = at.left, at.right, s - s // 4 * 2, (s + 2) % 6 if s < 4 else s - 4
            ka, kb = 1, 2
        self.wait(a, i)
        if s < 2:
            self.send(a, i, self.to_right.at[CHUNKS + s], at.right)
        self.wait(b, j)
        if s < 2:
            self.send(b, j, self.to_left.at[CHUNKS + s], at.left)
        if s == 1:
            between()
            self.right(2), self.left(0), self.right(3), self.left(1)
        self.send(a, i, self.to_sib.at[CHUNKS * ka + i], at.sib)
        self.send(b, j, self.to_sib.at[CHUNKS * kb + j], at.sib)
        return i, j

    def left_all(self):
        for sems, count in ((self.to_right, CHUNKS + 2), (self.to_left, CHUNKS + 2), (self.to_sib, 4 * CHUNKS)):
            for c in range(count):
                landed(self.piece(self.at.me, 0), sems.at[c])


def layer(n, x_hbm, gain_a_ref, wq_hbm, wk_hbm, wv_hbm, wo_hbm, gain_m_ref, wg_hbm, wu_hbm, wd_hbm, row_ref, block_ref, y_hbm,
          slots, hid_s, wo_s, wg_s, wu_s, wd_s, run_s, from_s, xh_s, top_s, mix_s,
          recv, to_right, to_left, to_sib, wo_recv, wo_right, wo_left, wo_over, wo_sib, all_send, all_recv,
          term_send, term_recv, ring_send, ring_recv, local, local_x):
    at = Place(n)
    me = at.me
    rows, d = xh_s.shape
    width = wq_hbm.shape[1]
    half, wide = rows // 2, d // 2
    q_at, k_at, seen_at, got_at = (i * width for i in range(4))
    tall = HEAD + 16

    g = Gather(at, slots, recv, to_right, to_left, to_sib)
    size = g.rows
    x_loads = [pltpu.make_async_copy(x_hbm.at[pl.ds(c * size, size), :], xh_s.at[pl.ds(c * size, size), :], local_x.at[c]) for c in range(CHUNKS)]
    loads = [pltpu.make_async_copy(w, wg_s.at[:, pl.ds(i * width, width)], local.at[i]) for i, w in enumerate((wq_hbm, wk_hbm, wv_hbm))]
    loads += [pltpu.make_async_copy(wo_hbm, wo_s.at[me], local.at[3]), pltpu.make_async_copy(wu_hbm, wu_s, local.at[4])]
    late = [pltpu.make_async_copy(wg_hbm, wg_s, local.at[5]), pltpu.make_async_copy(wd_hbm, wd_s, local.at[6])]
    for c in (0, 2, 1, 3):
        x_loads[c].start()
    for load in loads[:4]:
        load.start()
    barrier = pltpu.get_barrier_semaphore()
    for k in range(1, n):
        pl.semaphore_signal(barrier, inc=1, device_id={"tp": lax.rem(me + k, n)}, device_id_type=MESH)
    odd = lax.rem(lax.axis_index("dp"), 2)
    twin = {"dp": lax.axis_index("dp") + 1 - 2 * odd, "tp": me}
    pl.semaphore_signal(barrier, inc=1, device_id=twin, device_id_type=MESH)

    def norm(c, gain_ref):
        here = pl.ds(c * size, size)
        slots[me, here, :] = normed(xh_s[here, :], gain_ref[...])

    def first(c):
        x_loads[c].wait()
        norm(c, gain_a_ref)

    first(0)
    first(2)
    pl.semaphore_wait(barrier, n)
    g.start(lambda c: first(c) if c % 2 else None)
    for i in range(4):
        wd_s[i * tall + HEAD : (i + 1) * tall, :] = jnp.ones((tall - HEAD, d), jnp.bfloat16)
    for load in loads[:3]:
        load.wait()
    sign = jnp.where(lax.broadcasted_iota(jnp.int32, (1, HEAD), 1) < HEAD // 2, -1.0, 1.0)

    def value_at(h, b):
        return pl.multiple_of((2 * h + lax.div(b, n // 2)) * tall, 16), pl.multiple_of(lax.rem(b, n // 2) * rows, rows)

    def project(b, c):
        here = pl.ds(pl.multiple_of(c * size, size), size)
        a = slots[b, here, :]
        cr, sr = row_ref[0, here, :], row_ref[1, here, :]
        cb, sb = block_ref[0, pl.ds(b, 1), :], block_ref[1, pl.ds(b, 1), :]
        cos, sin = cr * cb - sr * sb, (sr * cb + cr * sb) * sign
        for w, out in ((0, q_at), (1, k_at)):
            t = dot(a, wg_s[:, w * width : (w + 1) * width]).astype(jnp.bfloat16).astype(jnp.float32)
            for h in range(2):
                one = t[:, h * HEAD : (h + 1) * HEAD]
                turned = one * cos + pltpu.roll(one, HEAD // 2, 1) * sin
                hid_s[b, here, out + h * HEAD : out + (h + 1) * HEAD] = turned.astype(jnp.bfloat16)
        t = dot(a, wg_s[:, 2 * width : 3 * width])
        for h in range(2):
            r, first = value_at(h, b)
            wd_s[pl.ds(r, HEAD), pl.ds(pl.multiple_of(first + c * size, size), size)] = t[:, h * HEAD : (h + 1) * HEAD].T.astype(jnp.bfloat16)

    for c in range(CHUNKS):
        g.wait(at.sib, c)
    lax.fori_loop(0, 2 * CHUNKS, lambda i, _: project(at.at(0, lax.div(i, CHUNKS)), lax.rem(i, CHUNKS)), None)

    lone, run = width // 4, width // 4

    def wo_rows(b, kind):
        if kind < 2:
            start, count = (lone * odd, width - run - lone * odd)[kind], run
        else:
            who = odd if kind > 3 else 1 - odd
            start, count = (run * who, width - lone - run * who)[kind % 2], lone
        return wo_s.at[b, pl.ds(pl.multiple_of(start, 16), count), :]

    def wo_send(b, kind, sem, device):
        sending(wo_rows(b, kind), wo_rows(b, kind), sem, wo_recv.at[b, kind], device).start()

    def wo_wait(b, kind):
        landed(wo_rows(b, kind), wo_recv.at[b, kind])

    def wo_first():
        loads[3].wait()
        wo_send(me, 0, wo_right.at[0], at.right)
        wo_send(me, 1, wo_left.at[0], at.left)

    def wo_cross(k, kind):
        b = (at.left, at.right, at.far)[k]
        piece = wo_rows(b, 4 + kind)
        pltpu.make_async_remote_copy(
            src_ref=piece, dst_ref=piece, send_sem=wo_over.at[k, kind], recv_sem=wo_recv.at[b, 2 + kind], device_id=twin, device_id_type=MESH
        ).start()
        wo_send(b, kind, wo_sib.at[1 + k, kind], at.sib)

    def wo_second():
        wo_send(me, 1, wo_right.at[1], at.right)
        wo_send(me, 0, wo_left.at[1], at.left)
        wo_wait(at.left, 0)
        wo_send(at.left, 0, wo_right.at[2], at.right)
        wo_wait(at.right, 1)
        wo_send(at.right, 1, wo_left.at[2], at.left)
        wo_cross(0, 0)
        wo_cross(1, 1)
        sending(wo_s.at[me], wo_s.at[me], wo_sib.at[0, 0], wo_recv.at[me, 0], at.sib).start()

    def wo_home(k, kind):
        b = (at.left, at.right, at.far)[k]
        wo_wait(b, 2 + kind)
        wo_send(b, 2 + kind, wo_sib.at[1 + k, 2 + kind], at.sib)

    def errands(u):
        @pl.when(u == 0)
        def _():
            wo_wait(at.left, 1)
            wo_cross(0, 1)
            wo_wait(at.right, 0)
            wo_cross(1, 0)

        @pl.when(u == 18)
        def _():
            for k, kind in ((0, 0), (1, 1), (0, 1), (1, 0)):
                wo_home(k, kind)

        @pl.when(u == 7)
        def _():
            for kind in range(2):
                wo_wait(at.far, kind)
                wo_cross(2, kind)

    e = HEAD**-0.5 * LOG2E
    part = rows // 2
    pieces = [(h, i) for h in range(2) for i in range(2)]

    def attend(key, b, slot, masked=False):
        keys = [(i + 1) * part if masked else rows for _, i in pieces]
        scores = [dot(hid_s[key, :count, k_at + h * HEAD : k_at + (h + 1) * HEAD],
                      hid_s[b, i * part : (i + 1) * part, q_at + h * HEAD : q_at + (h + 1) * HEAD], 1, 1) for (h, i), count in zip(pieces, keys)]
        weights, keeps = [], []
        for r, ((h, i), s) in enumerate(zip(pieces, scores)):
            if masked:
                ok = lax.broadcasted_iota(jnp.int32, s.shape, 1) + i * part >= lax.broadcasted_iota(jnp.int32, s.shape, 0)
                s = jnp.where(ok, s, HIDDEN)
            old = top_s[slot, r : r + 1, :]
            top = jnp.maximum(old, s.max(axis=0, keepdims=True))
            top_s[slot, r : r + 1, :] = top
            weights.append(jnp.exp2((s - top) * e).astype(jnp.bfloat16))
            keeps.append(jnp.exp2((old - top) * e))
        for r, ((h, i), p, keep, count) in enumerate(zip(pieces, weights, keeps, keys)):
            row, first = value_at(h, key)
            mix_s[slot, r] = mix_s[slot, r] * keep + dot(wd_s[pl.ds(row, HEAD + 8), pl.ds(first, count)], p)

    def clear(slot):
        top_s[slot] = jnp.full(top_s.shape[1:], NEG, jnp.float32)
        mix_s[slot] = jnp.zeros(mix_s.shape[1:], jnp.float32)

    def seen(b):
        return hid_s.at[b, :, pl.ds(seen_at, width)]

    def got(b):
        return hid_s.at[b, :, pl.ds(got_at, width)]

    def share(b):
        sending(seen(b), got(me), all_send.at[b], all_recv.at[me], b).start()

    def done(b, slot):
        for r, (h, i) in enumerate(pieces):
            m = mix_s[slot, r]
            o = m[:HEAD] * (1 / m[HEAD : HEAD + 1])
            hid_s[b, i * part : (i + 1) * part, seen_at + h * HEAD : seen_at + (h + 1) * HEAD] = o.T.astype(jnp.bfloat16)

    par = lax.rem(at.chip, 2)

    def key_of(m, p):
        return 2 * p + lax.div(m, 2) * 4 + lax.rem(m, 2)

    def early(i, _):
        b = key_of(i, par)
        clear(i)
        lax.fori_loop(0, i, lambda m, _: attend(key_of(m, par), b, i), None)
        attend(b, b, i, True)

    def sides(j, u):
        b = at.at(1 + (n // 2 - 2) * lax.rem(j, 2)) - at.core + lax.div(j, 2)
        clear(4)

        def one(m, _):
            attend(m, b, 4)
            errands(u + m)

        lax.fori_loop(0, b, one, None)
        attend(b, b, 4, True)
        errands(u + b)
        done(b, 4)
        share(b)
        return u + b + 1

    def across(j, u):
        chip = lax.rem(at.chip + 2 - lax.div(j, 2) * 2, n // 2)
        b = 2 * chip + lax.rem(j, 2)
        count = 2 * lax.div(chip + 1, 2)
        slot = 2 * lax.div(chip, 2) + lax.rem(j, 2)

        def one(m, _):
            attend(key_of(m, 1 - par), b, slot)
            errands(u + m)

        lax.fori_loop(0, count, one, None)
        done(b, slot)

        @pl.when(j < 2)
        def _():
            share(b)

        return u + count

    near = lambda side: n // 2 - 1 + 2 * side
    two = lambda side: 2
    for s in range(6):
        i, j = g.step(s, wo_first)
        if s == 1:
            loads[4].start()
        if s == 4:
            wo_second()
        off = two if s // 2 == 1 else near
        g.wait(at.at(off(0), 1), i)
        g.wait(at.at(off(1), 1), j)
        lax.fori_loop(0, 4, lambda k, _: project(at.at(off(lax.rem(k, 2)), lax.div(k, 2)), i + lax.rem(k, 2) * (j - i)), None)
        if s == 3:
            lax.fori_loop(0, 4, early, None)
    late[0].start()
    g.left_all()
    lax.fori_loop(2, 4, across, lax.fori_loop(0, 4, sides, lax.fori_loop(0, 2, across, 0)))
    late[1].start()

    share(at.sib)
    for kind in range(2):
        wo_home(2, kind)
    got(me)[...] = seen(me)[...]
    landed(wo_s.at[at.sib], wo_recv.at[at.sib, 0])
    for off in range(1, n // 2):
        for kind in range(4):
            wo_wait(at.at(off, 1), kind)
    for k in range(3):
        landed(wo_rows(me, 0), wo_right.at[k])
        landed(wo_rows(me, 0), wo_left.at[k])
        for kind in range(2):
            landed(wo_rows(me, 2), wo_over.at[k, kind])
            landed(wo_rows(me, 0), wo_sib.at[1 + k, kind])
            landed(wo_rows(me, 2), wo_sib.at[1 + k, 2 + kind])
    landed(wo_s.at[me], wo_sib.at[0, 0])
    for k in range(1, n):
        b = lax.rem(me + k, n)
        landed(got(b), all_recv.at[b])
    tile = 512

    def finish(c):
        here = pl.ds(c * size, size)

        def out(t, _):
            cols = pl.ds(pl.multiple_of(t * tile, tile), tile)
            total = dot(hid_s[0, here, got_at : got_at + width], wo_s[0, :, cols])
            for b in range(1, n):
                total += dot(hid_s[b, here, got_at : got_at + width], wo_s[b, :, cols])
            xh_s[here, cols] = (xh_s[here, cols].astype(jnp.float32) + total).astype(jnp.bfloat16)

        lax.fori_loop(0, d // tile, out, None)
        norm(c, gain_m_ref)

    g.start(finish)

    for k in range(1, n):
        b = lax.rem(me + k, n)
        landed(seen(b), all_send.at[b])
    loads[4].wait()
    late[0].wait()
    cut = 256
    cuts = hid_s.shape[2] // cut

    def hidden(b, part, t):
        here = pl.ds(pl.multiple_of(part * half, half), half)
        cols = pl.ds(pl.multiple_of(t * cut, cut), cut)
        a = slots[b, here, :]
        gate, up = dot(a, wg_s[:, cols]), dot(a, wu_s[:, cols])
        hid_s[b, here, cols] = (jax.nn.silu(gate) * up).astype(jnp.bfloat16)

    def four(off, part):
        def one(i, _):
            k, t = lax.div(i, cuts), lax.rem(i, cuts)
            side = lax.rem(k, 2)
            hidden(at.at(off(side), lax.div(k, 2)), part(side), t)
        lax.fori_loop(0, 4 * cuts, one, None)

    for c in range(CHUNKS):
        g.wait(at.sib, c)
    four(lambda side: 0, lambda side: side)

    def piece(ref, index, part, c):
        return ref.at[(*index, pl.ds(pl.multiple_of(part * half, half), half), pl.ds(pl.multiple_of(c * wide, wide), wide))]

    def term(b, part, c):
        rows_ = pl.ds(pl.multiple_of(part * half, half), half)
        return dot(hid_s[b, rows_, :], wd_s[:, pl.ds(pl.multiple_of(c * wide, wide), wide)])

    def give(k, off, part):
        def one(index, _):
            c, i = lax.div(index, 2), lax.rem(index, 2)
            other = at.at(off(i), 1)
            source = piece(slots, (other,), part(i), c)
            source[...] = term(other, part(i), c).astype(jnp.bfloat16)
            sending(source, piece(wo_s, (2 * k + i,), 0, c), term_send.at[k, i, c], term_recv.at[k, i, c], at.sib).start()

        lax.fori_loop(0, 4, one, None)

    def chips_term(k, off, part, i, c):
        mine = term(at.at(off), part, c)
        target = piece(wo_s, (2 * k + i,), 0, c)
        landed(target, term_recv.at[k, i, c])
        return mine + target[...].astype(jnp.float32)

    def group(k, off, part, stage, extra=False):
        give(k, off, part)

        def one(index, _):
            c, i = lax.div(index, 2), lax.rem(index, 2)
            total = chips_term(k, off(i), part(i), i, c)
            if extra:
                came = piece(run_s, (i,), 0, c)
                landed(came, ring_recv.at[1, i, c])
                total += came[...].astype(jnp.float32)
            source = piece(slots, (stage(i),), part(i), c)
            source[...] = total.astype(jnp.bfloat16)
            target = piece(run_s, (i,), 0, c) if k == 1 else piece(from_s, (i,), part(i), c)
            sending(source, target, ring_send.at[k, i, c], ring_recv.at[k, i, c], lax.rem(me + 2 + (n - 4) * i, n)).start()

        lax.fori_loop(0, 4, one, None)

    turned = lambda i: 1 + (n // 2 - 2) * i

    def pair(s):
        off = two if s // 2 == 1 else near
        i, j = ends[s]
        for c in (i - 1, i):
            g.wait(at.at(off(0), 1), c)
        for c in (j - 1, j):
            g.wait(at.at(off(1), 1), c)
        first, last = i // 2, j // 2
        four(off, lambda side: first + side * (last - first))

    ends = {}
    for s in range(6):
        ends[s] = g.step(s)
        if s == 1:
            pair(1)
            late[1].wait()
        elif s == 2:
            group(0, turned, lambda i: 1 - i, lambda i: at.sib)
        elif s == 3:
            pair(3)
        elif s == 4:
            g_far = lambda i: at.far
            for c in range(CHUNKS):
                landed(g.piece(me, 0), to_sib.at[3 * CHUNKS + c])
            group(1, two, lambda i: i, g_far)
        elif s == 5:
            pair(5)
    for sems, count in ((to_right, CHUNKS + 2), (to_left, CHUNKS + 2), (to_sib, 3 * CHUNKS)):
        for c in range(count):
            landed(g.piece(me, 0), sems.at[c])
    group(2, turned, lambda i: i, lambda i: at.at(turned(i)), extra=True)
    for i in range(2):
        for c in range(2):
            landed(piece(slots, (me,), 0, 0), ring_send.at[0, i, c])
    give(3, lambda i: 0, lambda i: i)

    def last(c, _):
        totals = [chips_term(3, 0, i, i, c) + piece(xh_s, (), i, c)[...].astype(jnp.float32) for i in range(2)]
        for i in range(2):
            total = totals[i]
            for side in range(2):
                came = piece(from_s, (side,), i, c)
                kind = 2 * (1 - i) if side == 0 else 2 * i
                landed(came, ring_recv.at[kind, side, c])
                total += came[...].astype(jnp.float32)
            source = piece(slots, (me,), i, c)
            source[...] = total.astype(jnp.bfloat16)
            pltpu.make_async_copy(source, piece(y_hbm, (), i, c), local_x.at[2 * c + i]).start()

    lax.fori_loop(0, 2, last, None)
    for i in range(2):
        for c in range(2):
            for k in range(4):
                landed(piece(slots, (me,), 0, 0), term_send.at[k, i, c])
            for k in range(1, 3):
                landed(piece(slots, (me,), 0, 0), ring_send.at[k, i, c])
            landed(piece(slots, (me,), 0, 0), local_x.at[2 * c + i])


def tables(rows, n):
    freq = float(THETA) ** (-np.arange(HEAD // 2) / (HEAD // 2))

    def both(place):
        angle = np.tile(place[:, None] * freq, (1, 2))
        return jnp.asarray(np.stack([np.cos(angle), np.sin(angle)]).astype(np.float32))

    return both(np.arange(rows)), both(np.arange(n) * rows)


def solution(mesh):
    n = mesh.shape["tp"]
    vmem, hbm = pl.BlockSpec(memory_space=pltpu.VMEM), pl.BlockSpec(memory_space=pl.ANY)
    dma = pltpu.SemaphoreType.DMA
    bf16 = jnp.bfloat16

    def step(x, gain_a, wq, wk, wv, wo, gain_m, w_gate, w_up, w_down):
        rows, d = x.shape
        width, units = wq.shape[1], w_gate.shape[1]
        row_table, block_table = tables(rows, n)
        return pl.pallas_call(
            functools.partial(layer, n),
            name="layer",
            out_shape=jax.ShapeDtypeStruct((rows, d), bf16),
            in_specs=[hbm, vmem, hbm, hbm, hbm, hbm, vmem, hbm, hbm, hbm, vmem, vmem],
            out_specs=hbm,
            scratch_shapes=[
                pltpu.VMEM((n, rows, d), bf16),
                pltpu.VMEM((n, rows, units), bf16),
                pltpu.VMEM((n, width, d), bf16),
                pltpu.VMEM((d, units), bf16),
                pltpu.VMEM((d, units), bf16),
                pltpu.VMEM((units, d), bf16),
                pltpu.VMEM((2, rows // 2, d), bf16),
                pltpu.VMEM((2, rows, d), bf16),
                pltpu.VMEM((rows, d), bf16),
                pltpu.VMEM((5, 4, rows // 2), jnp.float32),
                pltpu.VMEM((5, 4, HEAD + 8, rows // 2), jnp.float32),
                dma((n, CHUNKS)), dma((CHUNKS + 2,)), dma((CHUNKS + 2,)), dma((4 * CHUNKS,)),
                dma((n, 4)), dma((3,)), dma((3,)), dma((3, 2)), dma((4, 4)), dma((n,)), dma((n,)),
                dma((4, 2, 2)), dma((4, 2, 2)), dma((3, 2, 2)), dma((3, 2, 2)), dma((7,)), dma((CHUNKS,)),
            ],
            compiler_params=pltpu.CompilerParams(collective_id=0, has_side_effects=True, vmem_limit_bytes=LIMIT),
        )(x, gain_a, wq, wk, wv, wo, gain_m, w_gate, w_up, w_down, row_table, block_table)

    tokens, columns, rows_of = P(("dp", "tp"), None), P(None, "tp"), P("tp", None)
    return jax.shard_map(
        step,
        mesh=mesh,
        in_specs=(tokens, P(None), columns, columns, columns, rows_of, P(None), columns, columns, rows_of),
        out_specs=tokens,
        check_vma=False,
    )
```
